1024 devices in a mesh: er: 4 (over z_lo), ec: 4 (over z_hi), dp: 64 (over x, y, core).
Axes of the slice: x: 4, y: 8, z: 16 (z_hi: 4, z_lo: 4; z = z_hi * 4 + z_lo), core: 2. Of those that a mesh axis runs over, the one named last changes fastest.
Arguments:
- out_grad: bfloat16 [64, 1024, 4096], P('dp', 'er', 'ec'), may hold values from -6 to 6
- route_probs: float32 [64, 1024], P('dp', 'er'), may hold values from 0.1 to 1
- expert_ids: int32 [64, 1024], P('dp', 'er'), may hold values from 0 to 3, as said below
- slot_ids: int32 [64, 1024], P('dp', 'er'), may hold values from 0 to 71, as said below
- gate_pre: bfloat16 [64, 4, 288, 768], P('dp', 'er'), may hold values from -6 to 6
- up_act: bfloat16 [64, 4, 288, 768], P('dp', 'er'), may hold values from -6 to 6
- w_gate: bfloat16 [4, 4096, 768], P('er', 'ec'), may hold values from -0.09375 to 0.09375
- w_up: bfloat16 [4, 4096, 768], P('er', 'ec'), may hold values from -0.09375 to 0.09375
- w_down: bfloat16 [4, 768, 4096], P('er', None, 'ec'), may hold values from -0.21875 to 0.21875
Outputs:
- input_grad: bfloat16 [64, 1024, 4096], P('dp', 'er', 'ec')
- down_grad: float32 [4, 768, 4096], P('er', 'dp', 'ec')
The draws below stay inside these ranges and needn't reach their ends.
Inputs may be any that keep to these rules, and one draw needn't show every extreme that they name: `expert_ids`: within each group of 256 tokens no expert is chosen by more than 72 tokens; in every replica some expert is chosen by exactly 72 tokens of every group of that replica. `slot_ids`: tokens of one group that chose the same expert have distinct slots.
All inputs are finite; a program needn't handle non-finite values.
Results may differ from the reference program's by a relative error of at most 0.015.
Values may be sent and summed in bfloat16 or wider, within the bound.
A program may use at most 64 MiB of HBM per device.

```python
import jax
import jax.numpy as jnp
from jax import lax

D = 4096
H = 768
TOK = 256
C = 72
N_ER = 4
N_DP = 64


def route_table(key):

    def group_draw(replica, row_index):
        full_expert = jax.random.randint(jax.random.fold_in(jax.random.fold_in(key, 101), replica), (), 0, N_ER)
        group_key = jax.random.fold_in(jax.random.fold_in(key, 202), replica * N_ER + row_index)
        first_key, second_key = jax.random.split(group_key)
        ranking = jax.random.permutation(first_key, N_ER * C)
        slot_cells = jnp.arange(N_ER * C)
        scores = jnp.where(slot_cells // C == full_expert, ranking - N_ER * C, ranking)
        picked = jnp.argsort(scores, stable=True)[:TOK]
        picked = jax.random.permutation(second_key, picked)
        return (picked // C, picked % C)
    replicas = jnp.repeat(jnp.arange(N_DP), N_ER)
    row_values = jnp.tile(jnp.arange(N_ER), N_DP)
    chosen, placed = jax.vmap(group_draw)(replicas, row_values)
    return (chosen.reshape(N_DP, N_ER * TOK).astype(jnp.int32), placed.reshape(N_DP, N_ER * TOK).astype(jnp.int32))


def draw_expert_ids(key, part):
    return route_table(key)[0]


def draw_slot_ids(key, part):
    return route_table(key)[1]


def block_scale(own_key, shape, cuts, smallest, largest):
    loudness, own = 1.0, jax.random.fold_in(own_key, 6)
    for position, blocks in cuts:
        heights = jnp.exp(jax.random.uniform(jax.random.fold_in(own, position), (blocks,), jnp.float32, smallest / len(cuts), largest / len(cuts)))
        loudness = loudness * jnp.repeat(heights, shape[position] // blocks).reshape([-1 if axis == position else 1 for axis in range(len(shape))])
    return loudness


def normal_values(stream_key, shape, scale, bound, cuts=(), kind=jnp.bfloat16):
    array = jax.random.normal(stream_key, shape, jnp.float32) * scale
    if len(cuts) > 0:
        array = block_scale(stream_key, shape, cuts, -0.22, 0.18) * array
    return jnp.clip(array, min=-bound, max=bound).astype(kind)


def setup_inputs(seed: int = 0) -> dict:
    streams_of = jax.random.split(jax.random.key(seed), 10)
    out_grad = normal_values(streams_of[0], (N_DP, N_ER * TOK, D), 1.0, 6.0, ((0, 64), (1, 4), (2, 4)))
    route_probs = jnp.clip(0.1 + 0.9 * jax.random.uniform(streams_of[1], (N_DP, N_ER * TOK), jnp.float32) ** block_scale(streams_of[1], (N_DP, N_ER * TOK), ((0, 64), (1, 4)), -0.2, 0.2), 0.1, 1.0)
    expert_ids = draw_expert_ids(jax.random.fold_in(streams_of[9], 71), 0)
    slot_ids = draw_slot_ids(jax.random.fold_in(streams_of[9], 71), 0)
    gate_pre = normal_values(streams_of[4], (N_DP, N_ER, N_ER * C, H), 1.0, 6.0, ((0, 64), (1, 4)))
    up_act = normal_values(streams_of[5], (N_DP, N_ER, N_ER * C, H), 1.0, 6.0, ((0, 64), (1, 4)))
    w_gate = normal_values(streams_of[6], (N_ER, D, H), D ** -0.5, 0.09375, ((0, 4), (1, 4)))
    w_up = normal_values(streams_of[7], (N_ER, D, H), D ** -0.5, 0.09375, ((0, 4), (1, 4)))
    w_down = normal_values(streams_of[8], (N_ER, H, D), H ** -0.5, 0.21875, ((0, 4), (2, 4)))
    return {"out_grad": out_grad, "route_probs": route_probs, "expert_ids": expert_ids, "slot_ids": slot_ids, "gate_pre": gate_pre, "up_act": up_act, "w_gate": w_gate, "w_up": w_up, "w_down": w_down}


def reference(out_grad, route_probs, expert_ids, slot_ids, gate_pre, up_act, w_gate, w_up, w_down):
    slot_count = N_ER * C
    group_index = jnp.arange(N_ER * TOK, dtype=jnp.int32) // TOK

    def expert_step(pieces):
        slot_input, pre_rows, up_rows, gate_mat, up_mat, down_mat = pieces
        hid_grad = jnp.dot(slot_input, down_mat.T, preferred_element_type=jnp.float32)
        pre_float = pre_rows.astype(jnp.float32)
        up_float = up_rows.astype(jnp.float32)
        sigmoid = jax.nn.sigmoid(pre_float)
        gate_grad = (hid_grad * up_float * sigmoid * (1.0 + pre_float * (1.0 - sigmoid))).astype(jnp.bfloat16)
        up_grad = (hid_grad * pre_float * sigmoid).astype(jnp.bfloat16)
        hidden = (pre_float * sigmoid * up_float).astype(jnp.bfloat16)
        slot_grad = (jnp.dot(gate_grad, gate_mat.T, preferred_element_type=jnp.float32)
                     + jnp.dot(up_grad, up_mat.T, preferred_element_type=jnp.float32)).astype(jnp.bfloat16)
        weight_part = jnp.dot(hidden.T, slot_input, preferred_element_type=jnp.float32)
        return slot_grad, weight_part

    def replica(weight_total, inputs):
        grad_rows, prob_rows, expert_rows, slot_rows, pre_all, up_all = inputs
        scaled = (prob_rows[:, None] * grad_rows.astype(jnp.float32)).astype(jnp.bfloat16)
        target = (expert_rows * slot_count + group_index * C + slot_rows).astype(jnp.int32)
        placed = jnp.zeros((N_ER * slot_count, D), jnp.bfloat16).at[target].set(scaled)
        placed = placed.reshape(N_ER, slot_count, D)
        slot_grads, weight_parts = lax.map(expert_step, (placed, pre_all, up_all, w_gate, w_up, w_down))
        token_grads = slot_grads.reshape(N_ER * slot_count, D)[target]
        return weight_total + weight_parts, token_grads

    weight_total, input_grad = lax.scan(
        replica, jnp.zeros((N_ER, H, D), jnp.float32),
        (out_grad, route_probs, expert_ids, slot_ids, gate_pre, up_act))
    return input_grad, weight_total / N_DP
```

```python
import functools

import jax
import jax.numpy as jnp
from jax import lax
from jax.experimental import pallas as pl
from jax.experimental.pallas import tpu as pltpu
from jax.sharding import PartitionSpec as P

MESH = pl.DeviceIdType.MESH
F32, BF16 = jnp.float32, jnp.bfloat16
NX, NY, NC = 4, 8, 2
N = 4


def nt(a, b):
    return lax.dot_general(a, b, (((1,), (1,)), ((), ())), preferred_element_type=F32)


def kernel(
    tok_hbm, prob_ref, ids_ref, slots_ref, gate_hbm, up_hbm, wg_hbm, wu_hbm, wd_hbm,
    out_ref, down_ref,
    tok, gate, up, wg, wu, wd,
    outbuf, arrived, returned, slotbuf,
    gfac, ufac, hidden, hid_t,
    part, own, relay_in, direct_in, comb, comb_in, hid,
    dn, cin, xs, xin, ysum, ys, yin,
    lsem, disp_s, disp_r, rel_s, rel_r, dir_s, dir_r, com_s, com_r,
    aga_s, aga_r, agb_s, agb_r, agf_s, agf_r, ret_s, ret_r,
    core_s, core_r, x_s, x_r, y_s, y_r,
):
    e, c, p = lax.axis_index("er"), lax.axis_index("ec"), lax.axis_index("dp")
    core, y, x = p % NC, (p // NC) % NY, p // (NC * NY)
    cap = arrived.shape[1]
    half = part.shape[3]
    rows12 = ysum.shape[0] // NY

    def dp_at(x2, y2, core2):
        return (x2 * NY + y2) * NC + core2

    loads = [
        pltpu.make_async_copy(s, d, lsem.at[i])
        for i, (s, d) in enumerate(
            [(tok_hbm, tok), (gate_hbm, gate), (up_hbm, up), (wd_hbm, wd), (wg_hbm, wg), (wu_hbm, wu)]
        )
    ]
    for load in loads:
        load.start()

    right, left = {"ec": (c + 1) % N}, {"ec": (c + 3) % N}
    partners = [{"er": (e + k) % N} for k in (1, 2, 3)] + [right, left]
    partners += [{"dp": dp_at(x, y, 1 - core)}]
    partners += [{"dp": dp_at((x + k) % NX, y, core)} for k in range(1, NX)]
    partners += [{"dp": dp_at(x, (y + k) % NY, core)} for k in range(1, NY)]
    barrier = pltpu.get_barrier_semaphore()
    for partner in partners:
        pl.semaphore_signal(barrier, inc=1, device_id=partner, device_id_type=MESH)

    def remote(src, dst, s, r, dev):
        return pltpu.make_async_remote_copy(
            src_ref=src, dst_ref=dst, send_sem=s, recv_sem=r, device_id=dev, device_id_type=MESH
        )

    tokens = tok.shape[0]
    pos_row = ids_ref[...] * cap + slots_ref[...]
    eye = lax.broadcasted_iota(jnp.int32, (tokens, tokens), 0) == lax.broadcasted_iota(
        jnp.int32, (tokens, tokens), 1
    )

    def as_column(row):
        return jnp.sum(jnp.where(eye, jnp.broadcast_to(row, (tokens, tokens)), 0.0), axis=1, keepdims=True)

    prob_col = as_column(prob_ref[...])
    pos_col = as_column(pos_row.astype(F32))
    loads[0].wait()
    tok[...] = (prob_col * tok[...].astype(F32)).astype(BF16)
    for n, d in enumerate((2, 1, 3, 0)):
        dest = (c + d - e + 2 * N) % N
        k = (dest - e + N) % N
        slot = lax.broadcasted_iota(jnp.int32, (cap, tokens), 0) + dest * cap
        pick = jnp.where(slot == pos_row, 1.0, 0.0).astype(BF16)
        outbuf[d] = jnp.dot(pick, tok[...], preferred_element_type=F32).astype(BF16)
        if n == 0:
            pl.semaphore_wait(barrier, len(partners))

        @pl.when(k == 0)
        def _():
            arrived[e] = outbuf[d]

        @pl.when(k != 0)
        def _():
            remote(outbuf.at[d], arrived.at[e], disp_s.at[k - 1], disp_r.at[k - 1], {"er": dest}).start()

    loads[1].wait()
    loads[2].wait()

    def activations(r, _):
        a, u = gate[r].astype(F32), up[r].astype(F32)
        s = jax.nn.sigmoid(a)
        act = a * s
        ufac[r] = act
        gfac[r] = u * s * (1.0 + a * (1.0 - s))
        hidden[r] = (act * u).astype(BF16)
        return 0

    lax.fori_loop(0, N, activations, 0)
    mrows = hid_t.shape[2]
    width = hidden.shape[2]

    def arrange(q, _):
        row = q * mrows + lax.broadcasted_iota(jnp.int32, (mrows, width), 0)
        other = jnp.where(row >= width // 2, 1, 0)
        rem = row - other * (width // 2)
        group = ((rem.astype(F32) + 0.5) * (1.0 / rows12)).astype(jnp.int32)
        source = rem + rows12 * (group + other)
        pick = jnp.where(source == lax.broadcasted_iota(jnp.int32, (mrows, width), 1), 1.0, 0.0).astype(BF16)
        for r in range(N):
            hid_t[q, r] = nt(pick, hidden[r]).astype(BF16)
        return 0

    lax.fori_loop(0, NX * NC, arrange, 0)

    loads[3].wait()

    def partial(d):
        r = (c + d - e + 2 * N) % N
        k = (e - r + N) % N

        @pl.when(k != 0)
        def _():
            remote(outbuf.at[d], arrived.at[r], disp_s.at[k - 1], disp_r.at[k - 1], {"er": r}).wait_recv()

        return nt(arrived[r], wd[...])

    def keep(d, value):
        part[d, 0] = value[:, :half].astype(BF16)
        part[d, 1] = value[:, half:].astype(BF16)

    keep(2, partial(2))
    rel = [
        remote(part.at[2, 0], relay_in.at[0], rel_s.at[0], rel_r.at[0], right),
        remote(part.at[2, 1], relay_in.at[1], rel_s.at[1], rel_r.at[1], left),
    ]
    for copy in rel:
        copy.start()
    keep(1, partial(1))
    keep(3, partial(3))
    direct = [
        remote(part.at[3, 0], direct_in.at[0], dir_s.at[0], dir_r.at[0], left),
        remote(part.at[1, 1], direct_in.at[1], dir_s.at[1], dir_r.at[1], right),
    ]
    for copy in direct:
        copy.start()
    combined = []
    for h, (d, dev) in enumerate(((1, right), (3, left))):
        rel[h].wait_recv()
        comb[h] = (part[d, h].astype(F32) + relay_in[h].astype(F32)).astype(BF16)
        copy = remote(comb.at[h], comb_in.at[h], com_s.at[h], com_r.at[h], dev)
        copy.start()
        combined.append(copy)
    own[...] = partial(0)

    def outer(q, _):
        total = jnp.dot(hid_t[q, 0], arrived[0], preferred_element_type=F32)
        for r in range(1, N):
            total += jnp.dot(hid_t[q, r], arrived[r], preferred_element_type=F32)
        dn[q] = total.astype(BF16)
        return 0

    lax.fori_loop(0, NX * NC, outer, 0)
    swap = remote(
        dn.at[pl.ds((1 - core) * NX, NX)], cin, core_s, core_r, {"dp": dp_at(x, y, 1 - core)}
    )
    swap.start()

    for h in range(2):
        direct[h].wait_recv()
        combined[h].wait_recv()
        total = own[:, h * half : (h + 1) * half] + direct_in[h].astype(F32) + comb_in[h].astype(F32)
        hid[c, h] = total.astype(BF16)
    first = [
        remote(hid.at[c, 0], hid.at[c, 0], aga_s.at[0], aga_r.at[0], right),
        remote(hid.at[c, 1], hid.at[c, 1], aga_s.at[1], aga_r.at[1], left),
    ]
    second = [
        remote(hid.at[c, 0], hid.at[c, 0], agb_s.at[0], agb_r.at[0], left),
        remote(hid.at[c, 1], hid.at[c, 1], agb_s.at[1], agb_r.at[1], right),
    ]
    for copy in first + second:
        copy.start()

    loads[4].wait()
    loads[5].wait()

    def give_back(d):
        j = (c + d) % N
        r = (j - e + N) % N
        k = (r - e + N) % N
        value = None
        for h in range(2):
            cut = slice(h * half, (h + 1) * half)
            grad = hid[j, h].astype(F32)
            gate_grad = (grad * gfac[r, :, cut]).astype(BF16)
            up_grad = (grad * ufac[r, :, cut]).astype(BF16)
            term = nt(gate_grad, wg[:, cut]) + nt(up_grad, wu[:, cut])
            value = term if value is None else value + term
        slotbuf[d] = value.astype(BF16)

        @pl.when(k == 0)
        def _():
            returned[e] = slotbuf[d]

        @pl.when(k != 0)
        def _():
            remote(slotbuf.at[d], returned.at[e], ret_s.at[k - 1], ret_r.at[k - 1], {"er": r}).start()

    give_back(0)

    swap.wait_recv()
    for q in range(NX):
        xs[q] = (dn[core * NX + q].astype(F32) + cin[q].astype(F32)).astype(BF16)
    over_x = []
    for k in range(1, NX):
        x2 = (x + k) % NX
        copy = remote(
            xs.at[x2], xin.at[k - 1], x_s.at[k - 1], x_r.at[k - 1], {"dp": dp_at(x2, y, core)}
        )
        copy.start()
        over_x.append(copy)

    prev, nxt = (c + 3) % N, (c + 1) % N
    first[0].wait_recv()
    forward = [remote(hid.at[prev, 0], hid.at[prev, 0], agf_s.at[0], agf_r.at[0], right)]
    forward[0].start()
    first[1].wait_recv()
    forward.append(remote(hid.at[nxt, 1], hid.at[nxt, 1], agf_s.at[1], agf_r.at[1], left))
    forward[1].start()
    second[0].wait_recv()
    give_back(1)
    second[1].wait_recv()
    give_back(3)

    for copy in over_x:
        copy.wait_recv()
    total = dn[core * NX + x].astype(F32) + cin[x].astype(F32)
    for k in range(NX - 1):
        total += xin[k].astype(F32)
    ysum[...] = total
    for q in range(NY):
        ys[q] = ysum[q * rows12 : (q + 1) * rows12, :].astype(BF16)
    over_y = []
    for k in range(1, NY):
        y2 = (y + k) % NY
        copy = remote(
            ys.at[y2], yin.at[k - 1], y_s.at[k - 1], y_r.at[k - 1], {"dp": dp_at(x, y2, core)}
        )
        copy.start()
        over_y.append(copy)

    forward[0].wait_recv()
    forward[1].wait_recv()
    give_back(2)

    for copy in over_y:
        copy.wait_recv()
    total = ys[y].astype(F32)
    for k in range(NY - 1):
        total += yin[k].astype(F32)
    down_ref[...] = total * (1.0 / (NX * NY * NC))

    pos_lane = pos_col.astype(jnp.int32) - lax.broadcasted_iota(jnp.int32, (tokens, cap), 1)
    result = None
    for k in range(N):
        source = (e - k + N) % N
        if k > 0:
            remote(
                slotbuf.at[0], returned.at[source], ret_s.at[k - 1], ret_r.at[k - 1], {"er": source}
            ).wait_recv()
        pick = jnp.where(pos_lane == source * cap, 1.0, 0.0).astype(BF16)
        term = jnp.dot(pick, returned[source], preferred_element_type=F32)
        result = term if result is None else result + term
    out_ref[...] = result.astype(BF16)

    for k in range(N - 1):
        other = {"er": (e + k + 1) % N}
        remote(outbuf.at[0], arrived.at[e], disp_s.at[k], disp_r.at[k], other).wait_send()
        remote(slotbuf.at[0], returned.at[e], ret_s.at[k], ret_r.at[k], other).wait_send()
    for copy in rel + direct + combined + first + second + forward + over_x + over_y + [swap]:
        copy.wait_send()


def body(out_grad, route_probs, expert_ids, slot_ids, gate_pre, up_act, w_gate, w_up, w_down):
    tokens, cols = out_grad.shape[1:]
    slots, width = gate_pre.shape[2:]
    cap, half = slots // N, width // 2
    mrows = width // (NX * NC)
    rows12 = mrows // NY
    vmem, dma = pltpu.VMEM, pltpu.SemaphoreType.DMA
    scratch = [
        vmem((tokens, cols), BF16),
        vmem((N, cap, width), BF16),
        vmem((N, cap, width), BF16),
        vmem((cols, width), BF16),
        vmem((cols, width), BF16),
        vmem((width, cols), BF16),
        vmem((N, cap, cols), BF16),
        vmem((N, cap, cols), BF16),
        vmem((N, cap, cols), BF16),
        vmem((N, cap, cols), BF16),
        vmem((N, cap, width), F32),
        vmem((N, cap, width), F32),
        vmem((N, cap, width), BF16),
        vmem((NX * NC, N, mrows, cap), BF16),
        vmem((N, 2, cap, half), BF16),
        vmem((cap, width), F32),
        vmem((2, cap, half), BF16),
        vmem((2, cap, half), BF16),
        vmem((2, cap, half), BF16),
        vmem((2, cap, half), BF16),
        vmem((N, 2, cap, half), BF16),
        vmem((NX * NC, mrows, cols), BF16),
        vmem((NX, mrows, cols), BF16),
        vmem((NX, mrows, cols), BF16),
        vmem((NX - 1, mrows, cols), BF16),
        vmem((mrows, cols), F32),
        vmem((NY, rows12, cols), BF16),
        vmem((NY - 1, rows12, cols), BF16),
        dma((6,)),
        dma((N - 1,)),
        dma((N - 1,)),
        *[dma((2,)) for _ in range(12)],
        dma((N - 1,)),
        dma((N - 1,)),
        dma,
        dma,
        dma((NX - 1,)),
        dma((NX - 1,)),
        dma((NY - 1,)),
        dma((NY - 1,)),
    ]
    small = pl.BlockSpec(memory_space=pltpu.VMEM)
    big = pl.BlockSpec(memory_space=pl.ANY)
    input_grad, down_part = pl.pallas_call(
        kernel,
        out_shape=(
            jax.ShapeDtypeStruct((tokens, cols), BF16),
            jax.ShapeDtypeStruct((rows12, cols), F32),
        ),
        in_specs=[big, small, small, small, big, big, big, big, big],
        out_specs=(small, small),
        scratch_shapes=scratch,
        compiler_params=pltpu.CompilerParams(
            collective_id=0, has_side_effects=True, vmem_limit_bytes=48 * 1024 * 1024
        ),
        name="expert_backward",
    )(
        out_grad[0], route_probs, expert_ids, slot_ids,
        gate_pre.reshape(N, cap, width), up_act.reshape(N, cap, width),
        w_gate[0], w_up[0], w_down[0],
    )
    return (input_grad[None], down_part[None])


def solution(mesh):
    in_specs = (
        P("dp", "er", "ec"),
        P("dp", "er"),
        P("dp", "er"),
        P("dp", "er"),
        P("dp", "er", None, None),
        P("dp", "er", None, None),
        P("er", "ec", None),
        P("er", "ec", None),
        P("er", None, "ec"),
    )
    out_specs = (P("dp", "er", "ec"), P("er", "dp", "ec"))
    return jax.shard_map(body, mesh=mesh, in_specs=in_specs, out_specs=out_specs, check_vma=False)
```

```python
import functools

import jax
import jax.numpy as jnp
from jax import lax
from jax.experimental import pallas as pl
from jax.experimental.pallas import tpu as pltpu
from jax.sharding import PartitionSpec as P

MESH = pl.DeviceIdType.MESH
F32, BF16 = jnp.float32, jnp.bfloat16
NX, NY, NC = 4, 8, 2
N = 4


def nt(a, b):
    return lax.dot_general(a, b, (((1,), (1,)), ((), ())), preferred_element_type=F32)


def kernel(
    tok_hbm, prob_hbm, ids_hbm, slots_hbm, gate_hbm, up_hbm, wg_hbm, wu_hbm, wd_hbm,
    out_ref, down_ref,
    prob_ref, ids_ref, slots_ref,
    tok, gate, up, wg, wu, wd,
    outbuf, arrived, returned, slotbuf,
    gfac, ufac, hidden, hid_t,
    part, own, relay_in, direct_in, comb, comb_in, hid,
    dn, cin, xs, xin, ysum, ys, yin,
    lsem, disp_s, disp_r, rel_s, rel_r, dir_s, dir_r, com_s, com_r,
    aga_s, aga_r, agb_s, agb_r, agf_s, agf_r, ret_s, ret_r,
    core_s, core_r, x_s, x_r, y_s, y_r,
):
    e, c, p = lax.axis_index("er"), lax.axis_index("ec"), lax.axis_index("dp")
    core, y, x = p % NC, (p // NC) % NY, p // (NC * NY)
    cap = arrived.shape[1]
    half = part.shape[3]
    rows12 = ysum.shape[0] // NY

    def dp_at(x2, y2, core2):
        return (x2 * NY + y2) * NC + core2

    loads = [
        pltpu.make_async_copy(s, d, lsem.at[i])
        for i, (s, d) in enumerate(
            [
                (tok_hbm, tok), (gate_hbm, gate), (up_hbm, up), (wd_hbm, wd), (wg_hbm, wg), (wu_hbm, wu),
                (ids_hbm, ids_ref), (slots_hbm, slots_ref), (prob_hbm, prob_ref),
            ]
        )
    ]
    for i in (6, 7, 8, 0, 1, 2, 3, 4, 5):
        loads[i].start()

    right, left = {"ec": (c + 1) % N}, {"ec": (c + 3) % N}
    partners = [{"er": (e + k) % N} for k in (1, 2, 3)] + [right, left]
    partners += [{"dp": dp_at(x, y, 1 - core)}]
    partners += [{"dp": dp_at((x + k) % NX, y, core)} for k in range(1, NX)]
    partners += [{"dp": dp_at(x, (y + k) % NY, core)} for k in range(1, NY)]
    barrier = pltpu.get_barrier_semaphore()
    for partner in partners:
        pl.semaphore_signal(barrier, inc=1, device_id=partner, device_id_type=MESH)

    def remote(src, dst, s, r, dev):
        return pltpu.make_async_remote_copy(
            src_ref=src, dst_ref=dst, send_sem=s, recv_sem=r, device_id=dev, device_id_type=MESH
        )

    tokens = tok.shape[0]
    for i in (6, 7, 8):
        loads[i].wait()
    pos_row = ids_ref[...] * cap + slots_ref[...]
    eye = lax.broadcasted_iota(jnp.int32, (tokens, tokens), 0) == lax.broadcasted_iota(
        jnp.int32, (tokens, tokens), 1
    )

    def as_column(row):
        return jnp.sum(jnp.where(eye, jnp.broadcast_to(row, (tokens, tokens)), 0.0), axis=1, keepdims=True)

    prob_col = as_column(prob_ref[...])
    pos_col = as_column(pos_row.astype(F32))
    loads[0].wait()
    tok[...] = (prob_col * tok[...].astype(F32)).astype(BF16)
    for n, d in enumerate((2, 1, 3, 0)):
        dest = (c + d - e + 2 * N) % N
        k = (dest - e + N) % N
        slot = lax.broadcasted_iota(jnp.int32, (cap, tokens), 0) + dest * cap
        pick = jnp.where(slot == pos_row, 1.0, 0.0).astype(BF16)
        outbuf[d] = jnp.dot(pick, tok[...], preferred_element_type=F32).astype(BF16)
        if n == 0:
            pl.semaphore_wait(barrier, len(partners))

        @pl.when(k == 0)
        def _():
            arrived[e] = outbuf[d]

        @pl.when(k != 0)
        def _():
            remote(outbuf.at[d], arrived.at[e], disp_s.at[k - 1], disp_r.at[k - 1], {"er": dest}).start()

    loads[1].wait()
    loads[2].wait()

    def activations(r, _):
        a, u = gate[r].astype(F32), up[r].astype(F32)
        s = jax.nn.sigmoid(a)
        act = a * s
        ufac[r] = act
        gfac[r] = u * s * (1.0 + a * (1.0 - s))
        hidden[r] = (act * u).astype(BF16)
        return 0

    lax.fori_loop(0, N, activations, 0)
    mrows = hid_t.shape[2]
    width = hidden.shape[2]

    def arrange(q, _):
        row = q * mrows + lax.broadcasted_iota(jnp.int32, (mrows, width), 0)
        other = jnp.where(row >= width // 2, 1, 0)
        rem = row - other * (width // 2)
        group = ((rem.astype(F32) + 0.5) * (1.0 / rows12)).astype(jnp.int32)
        source = rem + rows12 * (group + other)
        pick = jnp.where(source == lax.broadcasted_iota(jnp.int32, (mrows, width), 1), 1.0, 0.0).astype(BF16)
        for r in range(N):
            hid_t[q, r] = nt(pick, hidden[r]).astype(BF16)
        return 0

    lax.fori_loop(0, NX * NC, arrange, 0)

    loads[3].wait()

    def partial(d):
        r = (c + d - e + 2 * N) % N
        k = (e - r + N) % N

        @pl.when(k != 0)
        def _():
            remote(outbuf.at[d], arrived.at[r], disp_s.at[k - 1], disp_r.at[k - 1], {"er": r}).wait_recv()

        return nt(arrived[r], wd[...])

    def keep(d, value):
        part[d, 0] = value[:, :half].astype(BF16)
        part[d, 1] = value[:, half:].astype(BF16)

    keep(2, partial(2))
    rel = [
        remote(part.at[2, 0], relay_in.at[0], rel_s.at[0], rel_r.at[0], right),
        remote(part.at[2, 1], relay_in.at[1], rel_s.at[1], rel_r.at[1], left),
    ]
    for copy in rel:
        copy.start()
    keep(1, partial(1))
    keep(3, partial(3))
    direct = [
        remote(part.at[3, 0], direct_in.at[0], dir_s.at[0], dir_r.at[0], left),
        remote(part.at[1, 1], direct_in.at[1], dir_s.at[1], dir_r.at[1], right),
    ]
    for copy in direct:
        copy.start()
    combined = []
    for h, (d, dev) in enumerate(((1, right), (3, left))):
        rel[h].wait_recv()
        comb[h] = (part[d, h].astype(F32) + relay_in[h].astype(F32)).astype(BF16)
        copy = remote(comb.at[h], comb_in.at[h], com_s.at[h], com_r.at[h], dev)
        copy.start()
        combined.append(copy)
    own[...] = partial(0)

    def outer(q, _):
        total = jnp.dot(hid_t[q, 0], arrived[0], preferred_element_type=F32)
        for r in range(1, N):
            total += jnp.dot(hid_t[q, r], arrived[r], preferred_element_type=F32)
        dn[q] = total.astype(BF16)
        return 0

    lax.fori_loop(0, NX * NC, outer, 0)
    swap = remote(
        dn.at[pl.ds((1 - core) * NX, NX)], cin, core_s, core_r, {"dp": dp_at(x, y, 1 - core)}
    )
    swap.start()

    swap.wait_recv()
    for q in range(NX):
        xs[q] = (dn[core * NX + q].astype(F32) + cin[q].astype(F32)).astype(BF16)
    over_x = []
    for k in range(1, NX):
        x2 = (x + k) % NX
        copy = remote(
            xs.at[x2], xin.at[k - 1], x_s.at[k - 1], x_r.at[k - 1], {"dp": dp_at(x2, y, core)}
        )
        copy.start()
        over_x.append(copy)

    for h in range(2):
        direct[h].wait_recv()
        combined[h].wait_recv()
        total = own[:, h * half : (h + 1) * half] + direct_in[h].astype(F32) + comb_in[h].astype(F32)
        hid[c, h] = total.astype(BF16)
    first = [
        remote(hid.at[c, 0], hid.at[c, 0], aga_s.at[0], aga_r.at[0], right),
        remote(hid.at[c, 1], hid.at[c, 1], aga_s.at[1], aga_r.at[1], left),
    ]
    second = [
        remote(hid.at[c, 0], hid.at[c, 0], agb_s.at[0], agb_r.at[0], left),
        remote(hid.at[c, 1], hid.at[c, 1], agb_s.at[1], agb_r.at[1], right),
    ]
    for copy in first + second:
        copy.start()

    loads[4].wait()
    loads[5].wait()

    def give_back(d):
        j = (c + d) % N
        r = (j - e + N) % N
        k = (r - e + N) % N
        value = None
        for h in range(2):
            cut = slice(h * half, (h + 1) * half)
            grad = hid[j, h].astype(F32)
            gate_grad = (grad * gfac[r, :, cut]).astype(BF16)
            up_grad = (grad * ufac[r, :, cut]).astype(BF16)
            term = nt(gate_grad, wg[:, cut]) + nt(up_grad, wu[:, cut])
            value = term if value is None else value + term
        slotbuf[d] = value.astype(BF16)

        @pl.when(k == 0)
        def _():
            returned[e] = slotbuf[d]

        @pl.when(k != 0)
        def _():
            remote(slotbuf.at[d], returned.at[e], ret_s.at[k - 1], ret_r.at[k - 1], {"er": r}).start()

    give_back(0)

    prev, nxt = (c + 3) % N, (c + 1) % N
    first[0].wait_recv()
    forward = [remote(hid.at[prev, 0], hid.at[prev, 0], agf_s.at[0], agf_r.at[0], right)]
    forward[0].start()
    first[1].wait_recv()
    forward.append(remote(hid.at[nxt, 1], hid.at[nxt, 1], agf_s.at[1], agf_r.at[1], left))
    forward[1].start()
    second[0].wait_recv()
    give_back(1)
    second[1].wait_recv()
    give_back(3)

    for copy in over_x:
        copy.wait_recv()
    total = dn[core * NX + x].astype(F32) + cin[x].astype(F32)
    for k in range(NX - 1):
        total += xin[k].astype(F32)
    ysum[...] = total
    for q in range(NY):
        ys[q] = ysum[q * rows12 : (q + 1) * rows12, :].astype(BF16)
    over_y = []
    for k in range(1, NY):
        y2 = (y + k) % NY
        copy = remote(
            ys.at[y2], yin.at[k - 1], y_s.at[k - 1], y_r.at[k - 1], {"dp": dp_at(x, y2, core)}
        )
        copy.start()
        over_y.append(copy)

    forward[0].wait_recv()
    forward[1].wait_recv()
    give_back(2)

    for copy in over_y:
        copy.wait_recv()
    total = ys[y].astype(F32)
    for k in range(NY - 1):
        total += yin[k].astype(F32)
    down_ref[...] = total * (1.0 / (NX * NY * NC))

    pos_lane = pos_col.astype(jnp.int32) - lax.broadcasted_iota(jnp.int32, (tokens, cap), 1)
    result = None
    for k in range(N):
        source = (e - k + N) % N
        if k > 0:
            remote(
                slotbuf.at[0], returned.at[source], ret_s.at[k - 1], ret_r.at[k - 1], {"er": source}
            ).wait_recv()
        pick = jnp.where(pos_lane == source * cap, 1.0, 0.0).astype(BF16)
        term = jnp.dot(pick, returned[source], preferred_element_type=F32)
        result = term if result is None else result + term
    out_ref[...] = result.astype(BF16)

    for k in range(N - 1):
        other = {"er": (e + k + 1) % N}
        remote(outbuf.at[0], arrived.at[e], disp_s.at[k], disp_r.at[k], other).wait_send()
        remote(slotbuf.at[0], returned.at[e], ret_s.at[k], ret_r.at[k], other).wait_send()
    for copy in rel + direct + combined + first + second + forward + over_x + over_y + [swap]:
        copy.wait_send()


def body(out_grad, route_probs, expert_ids, slot_ids, gate_pre, up_act, w_gate, w_up, w_down):
    tokens, cols = out_grad.shape[1:]
    slots, width = gate_pre.shape[2:]
    cap, half = slots // N, width // 2
    mrows = width // (NX * NC)
    rows12 = mrows // NY
    vmem, dma = pltpu.VMEM, pltpu.SemaphoreType.DMA
    scratch = [
        vmem((1, tokens), F32),
        vmem((1, tokens), jnp.int32),
        vmem((1, tokens), jnp.int32),
        vmem((tokens, cols), BF16),
        vmem((N, cap, width), BF16),
        vmem((N, cap, width), BF16),
        vmem((cols, width), BF16),
        vmem((cols, width), BF16),
        vmem((width, cols), BF16),
        vmem((N, cap, cols), BF16),
        vmem((N, cap, cols), BF16),
        vmem((N, cap, cols), BF16),
        vmem((N, cap, cols), BF16),
        vmem((N, cap, width), F32),
        vmem((N, cap, width), F32),
        vmem((N, cap, width), BF16),
        vmem((NX * NC, N, mrows, cap), BF16),
        vmem((N, 2, cap, half), BF16),
        vmem((cap, width), F32),
        vmem((2, cap, half), BF16),
        vmem((2, cap, half), BF16),
        vmem((2, cap, half), BF16),
        vmem((2, cap, half), BF16),
        vmem((N, 2, cap, half), BF16),
        vmem((NX * NC, mrows, cols), BF16),
        vmem((NX, mrows, cols), BF16),
        vmem((NX, mrows, cols), BF16),
        vmem((NX - 1, mrows, cols), BF16),
        vmem((mrows, cols), F32),
        vmem((NY, rows12, cols), BF16),
        vmem((NY - 1, rows12, cols), BF16),
        dma((9,)),
        dma((N - 1,)),
        dma((N - 1,)),
        *[dma((2,)) for _ in range(12)],
        dma((N - 1,)),
        dma((N - 1,)),
        dma,
        dma,
        dma((NX - 1,)),
        dma((NX - 1,)),
        dma((NY - 1,)),
        dma((NY - 1,)),
    ]
    small = pl.BlockSpec(memory_space=pltpu.VMEM)
    big = pl.BlockSpec(memory_space=pltpu.HBM)
    input_grad, down_part = pl.pallas_call(
        kernel,
        out_shape=(
            pltpu.VMEM((tokens, cols), BF16),
            pltpu.VMEM((rows12, cols), F32),
        ),
        in_specs=[big] * 9,
        out_specs=(small, small),
        scratch_shapes=scratch,
        compiler_params=pltpu.CompilerParams(
            collective_id=0, has_side_effects=True, vmem_limit_bytes=58 * 1024 * 1024
        ),
        name="expert_backward",
    )(
        out_grad[0], route_probs, expert_ids, slot_ids,
        gate_pre.reshape(N, cap, width), up_act.reshape(N, cap, width),
        w_gate[0], w_up[0], w_down[0],
    )
    return (input_grad[None], down_part[None])


def solution(mesh):
    in_specs = (
        P("dp", "er", "ec"),
        P("dp", "er"),
        P("dp", "er"),
        P("dp", "er"),
        P("dp", "er", None, None),
        P("dp", "er", None, None),
        P("er", "ec", None),
        P("er", "ec", None),
        P("er", None, "ec"),
    )
    out_specs = (P("dp", "er", "ec"), P("er", "dp", "ec"))
    return jax.shard_map(body, mesh=mesh, in_specs=in_specs, out_specs=out_specs, check_vma=False)
```

```python
import functools

import jax
import jax.numpy as jnp
from jax import lax
from jax.experimental import pallas as pl
from jax.experimental.pallas import tpu as pltpu
from jax.sharding import PartitionSpec as P

MESH = pl.DeviceIdType.MESH
F32, BF16 = jnp.float32, jnp.bfloat16
NX, NY, NC = 4, 8, 2
N = 4


def nt(a, b):
    return lax.dot_general(a, b, (((1,), (1,)), ((), ())), preferred_element_type=F32)


def kernel(
    tok_hbm, prob_hbm, ids_hbm, slots_hbm, gate_hbm, up_hbm, wg_hbm, wu_hbm, wd_hbm,
    out_ref, down_ref,
    prob_ref, ids_ref, slots_ref,
    tok, gate, up, wg, wu, wd,
    outbuf, arrived, returned, slotbuf,
    gfac, ufac, hidden, hid_t,
    part, own, relay_in, direct_in, comb, comb_in, hid,
    dn, cin, xs, xin, ysum, ys, yin,
    lsem, disp_s, disp_r, rel_s, rel_r, dir_s, dir_r, com_s, com_r,
    aga_s, aga_r, agb_s, agb_r, agf_s, agf_r, ret_s, ret_r,
    core_s, core_r, x_s, x_r, y_s, y_r,
):
    e, c, p = lax.axis_index("er"), lax.axis_index("ec"), lax.axis_index("dp")
    core, y, x = p % NC, (p // NC) % NY, p // (NC * NY)
    cap = arrived.shape[1]
    half = part.shape[3]
    rows12 = ysum.shape[0] // NY

    def dp_at(x2, y2, core2):
        return (x2 * NY + y2) * NC + core2

    loads = [
        pltpu.make_async_copy(s, d, lsem.at[i])
        for i, (s, d) in enumerate(
            [
                (tok_hbm, tok), (gate_hbm, gate), (up_hbm, up), (wd_hbm, wd), (wg_hbm, wg), (wu_hbm, wu),
                (ids_hbm, ids_ref), (slots_hbm, slots_ref), (prob_hbm, prob_ref),
            ]
        )
    ]
    for i in (6, 7, 8, 0, 1, 2, 3, 4, 5):
        loads[i].start()

    right, left = {"ec": (c + 1) % N}, {"ec": (c + 3) % N}
    partners = [{"er": (e + k) % N} for k in (1, 2, 3)] + [right, left]
    partners += [{"dp": dp_at(x, y, 1 - core)}]
    partners += [{"dp": dp_at((x + k) % NX, y, core)} for k in range(1, NX)]
    partners += [{"dp": dp_at(x, (y + k) % NY, core)} for k in range(1, NY)]
    barrier = pltpu.get_barrier_semaphore()
    for partner in partners:
        pl.semaphore_signal(barrier, inc=1, device_id=partner, device_id_type=MESH)

    def remote(src, dst, s, r, dev):
        return pltpu.make_async_remote_copy(
            src_ref=src, dst_ref=dst, send_sem=s, recv_sem=r, device_id=dev, device_id_type=MESH
        )

    def arriving(ref, r):
        remote(ref, ref, r, r, right).wait_recv()

    tokens = tok.shape[0]
    for i in (6, 7, 8):
        loads[i].wait()
    pos_row = ids_ref[...] * cap + slots_ref[...]
    eye = lax.broadcasted_iota(jnp.int32, (tokens, tokens), 0) == lax.broadcasted_iota(
        jnp.int32, (tokens, tokens), 1
    )

    def as_column(row):
        return jnp.sum(jnp.where(eye, jnp.broadcast_to(row, (tokens, tokens)), 0.0), axis=1, keepdims=True)

    prob_col = as_column(prob_ref[...])
    pos_col = as_column(pos_row.astype(F32))
    loads[0].wait()
    tok[...] = (prob_col * tok[...].astype(F32)).astype(BF16)
    for n, d in enumerate((2, 1, 3, 0)):
        dest = (c + d - e + 2 * N) % N
        k = (dest - e + N) % N
        slot = lax.broadcasted_iota(jnp.int32, (cap, tokens), 0) + dest * cap
        pick = jnp.where(slot == pos_row, 1.0, 0.0).astype(BF16)
        outbuf[d] = jnp.dot(pick, tok[...], preferred_element_type=F32).astype(BF16)
        if n == 0:
            pl.semaphore_wait(barrier, len(partners))

        @pl.when(k == 0)
        def _():
            arrived[e] = outbuf[d]

        @pl.when(k != 0)
        def _():
            remote(outbuf.at[d], arrived.at[e], disp_s.at[k - 1], disp_r.at[k - 1], {"er": dest}).start()

    loads[1].wait()
    loads[2].wait()

    def activations(r, _):
        a, u = gate[r].astype(F32), up[r].astype(F32)
        s = jax.nn.sigmoid(a)
        act = a * s
        ufac[r] = act
        gfac[r] = u * s * (1.0 + a * (1.0 - s))
        hidden[r] = (act * u).astype(BF16)
        return 0

    lax.fori_loop(0, N, activations, 0)
    mrows = hid_t.shape[2]
    width = hidden.shape[2]

    def arrange(q, _):
        row = q * mrows + lax.broadcasted_iota(jnp.int32, (mrows, width), 0)
        other = jnp.where(row >= width // 2, 1, 0)
        rem = row - other * (width // 2)
        group = ((rem.astype(F32) + 0.5) * (1.0 / rows12)).astype(jnp.int32)
        source = rem + rows12 * (group + other)
        pick = jnp.where(source == lax.broadcasted_iota(jnp.int32, (mrows, width), 1), 1.0, 0.0).astype(BF16)
        for r in range(N):
            hid_t[q, r] = nt(pick, hidden[r]).astype(BF16)
        return 0

    lax.fori_loop(0, NX * NC, arrange, 0)

    loads[3].wait()

    def partial(d):
        r = (c + d - e + 2 * N) % N
        k = (e - r + N) % N

        @pl.when(k != 0)
        def _():
            remote(outbuf.at[d], arrived.at[r], disp_s.at[k - 1], disp_r.at[k - 1], {"er": r}).wait_recv()

        return nt(arrived[r], wd[...])

    def keep(d, value):
        part[d, 0] = value[:, :half].astype(BF16)
        part[d, 1] = value[:, half:].astype(BF16)

    keep(2, partial(2))
    rel = [
        remote(part.at[2, 0], relay_in.at[0], rel_s.at[0], rel_r.at[0], right),
        remote(part.at[2, 1], relay_in.at[1], rel_s.at[1], rel_r.at[1], left),
    ]
    for copy in rel:
        copy.start()
    keep(1, partial(1))
    keep(3, partial(3))
    direct = [
        remote(part.at[3, 0], direct_in.at[0], dir_s.at[0], dir_r.at[0], left),
        remote(part.at[1, 1], direct_in.at[1], dir_s.at[1], dir_r.at[1], right),
    ]
    for copy in direct:
        copy.start()
    for n in range(2):
        h = jnp.where((c == 0) | (c == N - 1), 1 - n, n)
        d = 1 + 2 * h
        arriving(relay_in.at[h], rel_r.at[h])
        comb[h] = (part[d, h].astype(F32) + relay_in[h].astype(F32)).astype(BF16)
        remote(comb.at[h], comb_in.at[h], com_s.at[h], com_r.at[h], {"ec": (c + d) % N}).start()
    combined = [
        remote(comb.at[h], comb_in.at[h], com_s.at[h], com_r.at[h], dev) for h, dev in enumerate((right, left))
    ]
    own[...] = partial(0)

    def outer(q, _):
        total = jnp.dot(hid_t[q, 0], arrived[0], preferred_element_type=F32)
        for r in range(1, N):
            total += jnp.dot(hid_t[q, r], arrived[r], preferred_element_type=F32)
        dn[q] = total.astype(BF16)
        return 0

    lax.fori_loop(0, NX * NC, outer, 0)
    swap = remote(
        dn.at[pl.ds((1 - core) * NX, NX)], cin, core_s, core_r, {"dp": dp_at(x, y, 1 - core)}
    )
    swap.start()

    swap.wait_recv()
    for q in range(NX):
        xs[q] = (dn[core * NX + q].astype(F32) + cin[q].astype(F32)).astype(BF16)
    over_x = []
    for k in range(1, NX):
        x2 = (x + k) % NX
        copy = remote(
            xs.at[x2], xin.at[k - 1], x_s.at[k - 1], x_r.at[k - 1], {"dp": dp_at(x2, y, core)}
        )
        copy.start()
        over_x.append(copy)

    first = [
        remote(hid.at[c, 0], hid.at[c, 0], aga_s.at[0], aga_r.at[0], right),
        remote(hid.at[c, 1], hid.at[c, 1], aga_s.at[1], aga_r.at[1], left),
    ]
    second = [
        remote(hid.at[c, 0], hid.at[c, 0], agb_s.at[0], agb_r.at[0], left),
        remote(hid.at[c, 1], hid.at[c, 1], agb_s.at[1], agb_r.at[1], right),
    ]
    for h in range(2):
        direct[h].wait_recv()
        combined[h].wait_recv()
        total = own[:, h * half : (h + 1) * half] + direct_in[h].astype(F32) + comb_in[h].astype(F32)
        hid[c, h] = total.astype(BF16)
        first[h].start()
    for copy in second:
        copy.start()

    loads[4].wait()
    loads[5].wait()

    early = c < N // 2

    def give_back(d):
        j = (c + d) % N
        r = (j - e + N) % N
        k = (r - e + N) % N
        value = None
        for h in range(2):
            cut = slice(h * half, (h + 1) * half)
            grad = hid[j, h].astype(F32)
            gate_grad = (grad * gfac[r, :, cut]).astype(BF16)
            up_grad = (grad * ufac[r, :, cut]).astype(BF16)
            term = nt(gate_grad, wg[:, cut]) + nt(up_grad, wu[:, cut])
            value = term if value is None else value + term
        slotbuf[d] = value.astype(BF16)

        @pl.when(k == 0)
        def _():
            returned[e] = slotbuf[d]

        @pl.when((k != 0) & (early | (d == 2)))
        def _():
            send_back(d)

    def send_back(d):
        r = (c + d - e + N) % N
        k = (r - e + N) % N
        remote(slotbuf.at[d], returned.at[e], ret_s.at[k - 1], ret_r.at[k - 1], {"er": r}).start()

    give_back(0)

    for n in range(2):
        h = jnp.where((c == 1) | (c == 2), 1 - n, n)
        source = (c + 3 - 2 * h + N) % N
        arriving(hid.at[source, h], aga_r.at[h])
        remote(
            hid.at[source, h], hid.at[source, h], agf_s.at[h], agf_r.at[h], {"ec": (c + 1 + 2 * h) % N}
        ).start()
    forward = [
        remote(hid.at[(c + 2) % N, h], hid.at[(c + 2) % N, h], agf_s.at[h], agf_r.at[h], right) for h in range(2)
    ]
    for copy in over_x:
        copy.wait_recv()
    total = dn[core * NX + x].astype(F32) + cin[x].astype(F32)
    for k in range(NX - 1):
        total += xin[k].astype(F32)
    ysum[...] = total
    for q in range(NY):
        ys[q] = ysum[q * rows12 : (q + 1) * rows12, :].astype(BF16)
    over_y = []
    for k in range(1, NY):
        y2 = (y + k) % NY
        copy = remote(
            ys.at[y2], yin.at[k - 1], y_s.at[k - 1], y_r.at[k - 1], {"dp": dp_at(x, y2, core)}
        )
        copy.start()
        over_y.append(copy)

    second[0].wait_recv()
    give_back(1)
    second[1].wait_recv()
    give_back(3)

    forward[0].wait_recv()
    forward[1].wait_recv()
    for d in (0, 1, 3):

        @pl.when(jnp.logical_not(early) & ((c + d - 2 * e + 2 * N) % N != 0))
        def _():
            send_back(d)

    give_back(2)

    for copy in over_y:
        copy.wait_recv()
    total = ys[y].astype(F32)
    for k in range(NY - 1):
        total += yin[k].astype(F32)
    down_ref[...] = total * (1.0 / (NX * NY * NC))

    pos_lane = pos_col.astype(jnp.int32) - lax.broadcasted_iota(jnp.int32, (tokens, cap), 1)
    result = None
    for k in range(N):
        source = (e - k + N) % N
        if k > 0:
            remote(
                slotbuf.at[0], returned.at[source], ret_s.at[k - 1], ret_r.at[k - 1], {"er": source}
            ).wait_recv()
        pick = jnp.where(pos_lane == source * cap, 1.0, 0.0).astype(BF16)
        term = jnp.dot(pick, returned[source], preferred_element_type=F32)
        result = term if result is None else result + term
    out_ref[...] = result.astype(BF16)

    for k in range(N - 1):
        other = {"er": (e + k + 1) % N}
        remote(outbuf.at[0], arrived.at[e], disp_s.at[k], disp_r.at[k], other).wait_send()
        remote(slotbuf.at[0], returned.at[e], ret_s.at[k], ret_r.at[k], other).wait_send()
    for copy in rel + direct + combined + first + second + forward + over_x + over_y + [swap]:
        copy.wait_send()


def body(out_grad, route_probs, expert_ids, slot_ids, gate_pre, up_act, w_gate, w_up, w_down):
    tokens, cols = out_grad.shape[1:]
    slots, width = gate_pre.shape[2:]
    cap, half = slots // N, width // 2
    mrows = width // (NX * NC)
    rows12 = mrows // NY
    vmem, dma = pltpu.VMEM, pltpu.SemaphoreType.DMA
    scratch = [
        vmem((1, tokens), F32),
        vmem((1, tokens), jnp.int32),
        vmem((1, tokens), jnp.int32),
        vmem((tokens, cols), BF16),
        vmem((N, cap, width), BF16),
        vmem((N, cap, width), BF16),
        vmem((cols, width), BF16),
        vmem((cols, width), BF16),
        vmem((width, cols), BF16),
        vmem((N, cap, cols), BF16),
        vmem((N, cap, cols), BF16),
        vmem((N, cap, cols), BF16),
        vmem((N, cap, cols), BF16),
        vmem((N, cap, width), F32),
        vmem((N, cap, width), F32),
        vmem((N, cap, width), BF16),
        vmem((NX * NC, N, mrows, cap), BF16),
        vmem((N, 2, cap, half), BF16),
        vmem((cap, width), F32),
        vmem((2, cap, half), BF16),
        vmem((2, cap, half), BF16),
        vmem((2, cap, half), BF16),
        vmem((2, cap, half), BF16),
        vmem((N, 2, cap, half), BF16),
        vmem((NX * NC, mrows, cols), BF16),
        vmem((NX, mrows, cols), BF16),
        vmem((NX, mrows, cols), BF16),
        vmem((NX - 1, mrows, cols), BF16),
        vmem((mrows, cols), F32),
        vmem((NY, rows12, cols), BF16),
        vmem((NY - 1, rows12, cols), BF16),
        dma((9,)),
        dma((N - 1,)),
        dma((N - 1,)),
        *[dma((2,)) for _ in range(12)],
        dma((N - 1,)),
        dma((N - 1,)),
        dma,
        dma,
        dma((NX - 1,)),
        dma((NX - 1,)),
        dma((NY - 1,)),
        dma((NY - 1,)),
    ]
    small = pl.BlockSpec(memory_space=pltpu.VMEM)
    big = pl.BlockSpec(memory_space=pltpu.HBM)
    input_grad, down_part = pl.pallas_call(
        kernel,
        out_shape=(
            pltpu.VMEM((tokens, cols), BF16),
            pltpu.VMEM((rows12, cols), F32),
        ),
        in_specs=[big] * 9,
        out_specs=(small, small),
        scratch_shapes=scratch,
        compiler_params=pltpu.CompilerParams(
            collective_id=0, has_side_effects=True, vmem_limit_bytes=58 * 1024 * 1024
        ),
        name="expert_backward",
    )(
        out_grad[0], route_probs, expert_ids, slot_ids,
        gate_pre.reshape(N, cap, width), up_act.reshape(N, cap, width),
        w_gate[0], w_up[0], w_down[0],
    )
    return (input_grad[None], down_part[None])


def solution(mesh):
    in_specs = (
        P("dp", "er", "ec"),
        P("dp", "er"),
        P("dp", "er"),
        P("dp", "er"),
        P("dp", "er", None, None),
        P("dp", "er", None, None),
        P("er", "ec", None),
        P("er", "ec", None),
        P("er", None, "ec"),
    )
    out_specs = (P("dp", "er", "ec"), P("er", "dp", "ec"))
    return jax.shard_map(body, mesh=mesh, in_specs=in_specs, out_specs=out_specs, check_vma=False)
```

```python
import functools

import jax
import jax.numpy as jnp
from jax import lax
from jax.experimental import pallas as pl
from jax.experimental.pallas import tpu as pltpu
from jax.sharding import PartitionSpec as P

MESH = pl.DeviceIdType.MESH
F32, BF16 = jnp.float32, jnp.bfloat16
NX, NY, NC = 4, 8, 2
LIMIT = 58 * 1024 * 1024
N = 4


def nt(a, b):
    return lax.dot_general(a, b, (((1,), (1,)), ((), ())), preferred_element_type=F32)


def remote(src, dst, s, r, dev):
    return pltpu.make_async_remote_copy(
        src_ref=src, dst_ref=dst, send_sem=s, recv_sem=r, device_id=dev, device_id_type=MESH
    )


def greet(partners):
    barrier = pltpu.get_barrier_semaphore()
    for partner in partners:
        pl.semaphore_signal(barrier, inc=1, device_id=partner, device_id_type=MESH)
    return barrier


def copies_in(pairs, sems):
    loads = [pltpu.make_async_copy(s, d, sems.at[i]) for i, (s, d) in enumerate(pairs)]
    for load in loads:
        load.start()
    return loads


def as_column(row):
    n = row.shape[1]
    eye = lax.broadcasted_iota(jnp.int32, (n, n), 0) == lax.broadcasted_iota(jnp.int32, (n, n), 1)
    return jnp.sum(jnp.where(eye, jnp.broadcast_to(row, (n, n)), 0.0), axis=1, keepdims=True)


def dispatch_kernel(
    tok_hbm, prob_hbm, ids_hbm, slots_hbm, gate_hbm, up_hbm,
    arrived, gfac, ufac, hid_t, place,
    prob_ref, ids_ref, slots_ref, tok, gate, up, outbuf, hidden,
    lsem, disp_s, disp_r,
):
    e, c = lax.axis_index("er"), lax.axis_index("ec")
    cap = arrived.shape[1]
    rows12 = hid_t.shape[2] // NY
    loads = copies_in(
        [
            (ids_hbm, ids_ref), (slots_hbm, slots_ref), (prob_hbm, prob_ref),
            (tok_hbm, tok), (gate_hbm, gate), (up_hbm, up),
        ],
        lsem,
    )
    others = [{"er": (e + k) % N} for k in range(1, N)]
    barrier = greet(others)
    tokens = tok.shape[0]
    for i in range(3):
        loads[i].wait()
    pos_row = ids_ref[...] * cap + slots_ref[...]
    place[...] = pos_row.astype(F32)
    prob_col = as_column(prob_ref[...])
    loads[3].wait()
    tok[...] = (prob_col * tok[...].astype(F32)).astype(BF16)
    for n, d in enumerate((2, 1, 3, 0)):
        dest = (c + d - e + 2 * N) % N
        k = (dest - e + N) % N
        slot = lax.broadcasted_iota(jnp.int32, (cap, tokens), 0) + dest * cap
        pick = jnp.where(slot == pos_row, 1.0, 0.0).astype(BF16)
        outbuf[d] = jnp.dot(pick, tok[...], preferred_element_type=F32).astype(BF16)
        if n == 0:
            pl.semaphore_wait(barrier, len(others))

        @pl.when(k == 0)
        def _():
            arrived[e] = outbuf[d]

        @pl.when(k != 0)
        def _():
            remote(outbuf.at[d], arrived.at[e], disp_s.at[k - 1], disp_r.at[k - 1], {"er": dest}).start()

    loads[4].wait()
    loads[5].wait()

    def activations(r, _):
        a, u = gate[r].astype(F32), up[r].astype(F32)
        s = jax.nn.sigmoid(a)
        act = a * s
        ufac[r] = act
        gfac[r] = u * s * (1.0 + a * (1.0 - s))
        hidden[r] = (act * u).astype(BF16)
        return 0

    lax.fori_loop(0, N, activations, 0)
    mrows = hid_t.shape[2]
    width = hidden.shape[2]

    def arrange(q, _):
        row = q * mrows + lax.broadcasted_iota(jnp.int32, (mrows, width), 0)
        other = jnp.where(row >= width // 2, 1, 0)
        rem = row - other * (width // 2)
        group = ((rem.astype(F32) + 0.5) * (1.0 / rows12)).astype(jnp.int32)
        source = rem + rows12 * (group + other)
        pick = jnp.where(source == lax.broadcasted_iota(jnp.int32, (mrows, width), 1), 1.0, 0.0).astype(BF16)
        for r in range(N):
            hid_t[q, r] = nt(pick, hidden[r]).astype(BF16)
        return 0

    lax.fori_loop(0, NX * NC, arrange, 0)

    for k in range(N - 1):
        source = (e - k - 1 + N) % N
        remote(outbuf.at[0], arrived.at[source], disp_s.at[k], disp_r.at[k], others[k]).wait()


def kernel(
    arrived, gfac, ufac, hid_t, place, wg_hbm, wu_hbm, wd_hbm,
    out_ref, down_ref,
    wg, wu, wd,
    returned, slotbuf,
    part, own, relay_in, direct_in, comb, comb_in, hid,
    dn, cin, xs, xin, ysum, ys, yin,
    lsem, rel_s, rel_r, dir_s, dir_r, com_s, com_r,
    aga_s, aga_r, agb_s, agb_r, agf_s, agf_r, ret_s, ret_r,
    core_s, core_r, x_s, x_r, y_s, y_r,
):
    e, c, p = lax.axis_index("er"), lax.axis_index("ec"), lax.axis_index("dp")
    core, y, x = p % NC, (p // NC) % NY, p // (NC * NY)
    cap = arrived.shape[1]
    half = part.shape[3]
    rows12 = ysum.shape[0] // NY
    tokens = out_ref.shape[0]

    def dp_at(x2, y2, core2):
        return (x2 * NY + y2) * NC + core2

    loads = copies_in(
        [(wd_hbm, wd), (wg_hbm, wg), (wu_hbm, wu)], lsem
    )
    right, left = {"ec": (c + 1) % N}, {"ec": (c + 3) % N}
    partners = [{"er": (e + k) % N} for k in (1, 2, 3)] + [right, left]
    partners += [{"dp": dp_at(x, y, 1 - core)}]
    partners += [{"dp": dp_at((x + k) % NX, y, core)} for k in range(1, NX)]
    partners += [{"dp": dp_at(x, (y + k) % NY, core)} for k in range(1, NY)]
    barrier = greet(partners)

    def arriving(ref, r):
        remote(ref, ref, r, r, right).wait_recv()

    loads[0].wait()

    def partial(d):
        return nt(arrived[(c + d - e + 2 * N) % N], wd[...])

    def keep(d, value):
        part[d, 0] = value[:, :half].astype(BF16)
        part[d, 1] = value[:, half:].astype(BF16)

    keep(2, partial(2))
    pos_col = as_column(place[...])
    pl.semaphore_wait(barrier, len(partners))
    rel = [
        remote(part.at[2, 0], relay_in.at[0], rel_s.at[0], rel_r.at[0], right),
        remote(part.at[2, 1], relay_in.at[1], rel_s.at[1], rel_r.at[1], left),
    ]
    for copy in rel:
        copy.start()
    keep(1, partial(1))
    keep(3, partial(3))
    direct = [
        remote(part.at[3, 0], direct_in.at[0], dir_s.at[0], dir_r.at[0], left),
        remote(part.at[1, 1], direct_in.at[1], dir_s.at[1], dir_r.at[1], right),
    ]
    for copy in direct:
        copy.start()
    for n in range(2):
        h = jnp.where((c == 0) | (c == N - 1), 1 - n, n)
        d = 1 + 2 * h
        arriving(relay_in.at[h], rel_r.at[h])
        comb[h] = (part[d, h].astype(F32) + relay_in[h].astype(F32)).astype(BF16)
        remote(comb.at[h], comb_in.at[h], com_s.at[h], com_r.at[h], {"ec": (c + d) % N}).start()
    combined = [
        remote(comb.at[h], comb_in.at[h], com_s.at[h], com_r.at[h], dev) for h, dev in enumerate((right, left))
    ]
    own[...] = partial(0)

    def outer(q, _):
        total = jnp.dot(hid_t[q, 0], arrived[0], preferred_element_type=F32)
        for r in range(1, N):
            total += jnp.dot(hid_t[q, r], arrived[r], preferred_element_type=F32)
        dn[q] = total.astype(BF16)
        return 0

    lax.fori_loop(0, NX * NC, outer, 0)
    swap = remote(
        dn.at[pl.ds((1 - core) * NX, NX)], cin, core_s, core_r, {"dp": dp_at(x, y, 1 - core)}
    )
    swap.start()

    swap.wait_recv()
    for q in range(NX):
        xs[q] = (dn[core * NX + q].astype(F32) + cin[q].astype(F32)).astype(BF16)
    over_x = []
    for k in range(1, NX):
        x2 = (x + k) % NX
        copy = remote(
            xs.at[x2], xin.at[k - 1], x_s.at[k - 1], x_r.at[k - 1], {"dp": dp_at(x2, y, core)}
        )
        copy.start()
        over_x.append(copy)

    first = [
        remote(hid.at[c, 0], hid.at[c, 0], aga_s.at[0], aga_r.at[0], right),
        remote(hid.at[c, 1], hid.at[c, 1], aga_s.at[1], aga_r.at[1], left),
    ]
    second = [
        remote(hid.at[c, 0], hid.at[c, 0], agb_s.at[0], agb_r.at[0], left),
        remote(hid.at[c, 1], hid.at[c, 1], agb_s.at[1], agb_r.at[1], right),
    ]
    for h in range(2):
        direct[h].wait_recv()
        combined[h].wait_recv()
        total = own[:, h * half : (h + 1) * half] + direct_in[h].astype(F32) + comb_in[h].astype(F32)
        hid[c, h] = total.astype(BF16)
        first[h].start()
    for copy in second:
        copy.start()

    loads[1].wait()
    loads[2].wait()

    early = c < N // 2

    def give_back(d):
        j = (c + d) % N
        r = (j - e + N) % N
        k = (r - e + N) % N
        value = None
        for h in range(2):
            cut = slice(h * half, (h + 1) * half)
            grad = hid[j, h].astype(F32)
            gate_grad = (grad * gfac[r, :, cut]).astype(BF16)
            up_grad = (grad * ufac[r, :, cut]).astype(BF16)
            term = nt(gate_grad, wg[:, cut]) + nt(up_grad, wu[:, cut])
            value = term if value is None else value + term
        slotbuf[d] = value.astype(BF16)

        @pl.when(k == 0)
        def _():
            returned[e] = slotbuf[d]

        @pl.when((k != 0) & (early | (d == 2)))
        def _():
            send_back(d)

    def send_back(d):
        r = (c + d - e + N) % N
        k = (r - e + N) % N
        remote(slotbuf.at[d], returned.at[e], ret_s.at[k - 1], ret_r.at[k - 1], {"er": r}).start()

    give_back(0)

    for n in range(2):
        h = jnp.where((c == 1) | (c == 2), 1 - n, n)
        source = (c + 3 - 2 * h + N) % N
        arriving(hid.at[source, h], aga_r.at[h])
        remote(
            hid.at[source, h], hid.at[source, h], agf_s.at[h], agf_r.at[h], {"ec": (c + 1 + 2 * h) % N}
        ).start()
    forward = [
        remote(hid.at[(c + 2) % N, h], hid.at[(c + 2) % N, h], agf_s.at[h], agf_r.at[h], right) for h in range(2)
    ]
    for copy in over_x:
        copy.wait_recv()
    total = dn[core * NX + x].astype(F32) + cin[x].astype(F32)
    for k in range(NX - 1):
        total += xin[k].astype(F32)
    ysum[...] = total
    for q in range(NY):
        ys[q] = ysum[q * rows12 : (q + 1) * rows12, :].astype(BF16)
    over_y = []
    for k in range(1, NY):
        y2 = (y + k) % NY
        copy = remote(
            ys.at[y2], yin.at[k - 1], y_s.at[k - 1], y_r.at[k - 1], {"dp": dp_at(x, y2, core)}
        )
        copy.start()
        over_y.append(copy)

    second[0].wait_recv()
    give_back(1)
    second[1].wait_recv()
    give_back(3)

    forward[0].wait_recv()
    forward[1].wait_recv()
    for d in (0, 1, 3):

        @pl.when(jnp.logical_not(early) & ((c + d - 2 * e + 2 * N) % N != 0))
        def _():
            send_back(d)

    give_back(2)

    for copy in over_y:
        copy.wait_recv()
    total = ys[y].astype(F32)
    for k in range(NY - 1):
        total += yin[k].astype(F32)
    down_ref[...] = total * (1.0 / (NX * NY * NC))

    pos_lane = pos_col.astype(jnp.int32) - lax.broadcasted_iota(jnp.int32, (tokens, cap), 1)
    result = None
    for k in range(N):
        source = (e - k + N) % N
        if k > 0:
            remote(
                slotbuf.at[0], returned.at[source], ret_s.at[k - 1], ret_r.at[k - 1], {"er": source}
            ).wait_recv()
        pick = jnp.where(pos_lane == source * cap, 1.0, 0.0).astype(BF16)
        term = jnp.dot(pick, returned[source], preferred_element_type=F32)
        result = term if result is None else result + term
    out_ref[...] = result.astype(BF16)

    for k in range(N - 1):
        other = {"er": (e + k + 1) % N}
        remote(slotbuf.at[0], returned.at[e], ret_s.at[k], ret_r.at[k], other).wait_send()
    for copy in rel + direct + combined + first + second + forward + over_x + over_y + [swap]:
        copy.wait_send()


def body(out_grad, route_probs, expert_ids, slot_ids, gate_pre, up_act, w_gate, w_up, w_down):
    tokens, cols = out_grad.shape[1:]
    slots, width = gate_pre.shape[2:]
    cap, half = slots // N, width // 2
    mrows = width // (NX * NC)
    rows12 = mrows // NY
    vmem, dma = pltpu.VMEM, pltpu.SemaphoreType.DMA
    small = pl.BlockSpec(memory_space=pltpu.VMEM)
    big = pl.BlockSpec(memory_space=pl.ANY)
    handed = pl.pallas_call(
        dispatch_kernel,
        out_shape=(
            vmem((N, cap, cols), BF16),
            vmem((N, cap, width), F32),
            vmem((N, cap, width), F32),
            vmem((NX * NC, N, mrows, cap), BF16),
            vmem((1, tokens), F32),
        ),
        in_specs=[big] * 6,
        out_specs=(small,) * 5,
        scratch_shapes=[
            vmem((1, tokens), F32),
            vmem((1, tokens), jnp.int32),
            vmem((1, tokens), jnp.int32),
            vmem((tokens, cols), BF16),
            vmem((N, cap, width), BF16),
            vmem((N, cap, width), BF16),
            vmem((N, cap, cols), BF16),
            vmem((N, cap, width), BF16),
            dma((6,)),
            dma((N - 1,)),
            dma((N - 1,)),
        ],
        compiler_params=pltpu.CompilerParams(
            collective_id=1, has_side_effects=True, vmem_limit_bytes=LIMIT
        ),
        name="dispatch",
    )(
        out_grad[0], route_probs, expert_ids, slot_ids,
        gate_pre.reshape(N, cap, width), up_act.reshape(N, cap, width),
    )
    scratch = [
        vmem((cols, width), BF16),
        vmem((cols, width), BF16),
        vmem((width, cols), BF16),
        vmem((N, cap, cols), BF16),
        vmem((N, cap, cols), BF16),
        vmem((N, 2, cap, half), BF16),
        vmem((cap, width), F32),
        *[vmem((2, cap, half), BF16) for _ in range(4)],
        vmem((N, 2, cap, half), BF16),
        vmem((NX * NC, mrows, cols), BF16),
        vmem((NX, mrows, cols), BF16),
        vmem((NX, mrows, cols), BF16),
        vmem((NX - 1, mrows, cols), BF16),
        vmem((mrows, cols), F32),
        vmem((NY, rows12, cols), BF16),
        vmem((NY - 1, rows12, cols), BF16),
        dma((3,)),
        *[dma((2,)) for _ in range(12)],
        dma((N - 1,)),
        dma((N - 1,)),
        dma,
        dma,
        dma((NX - 1,)),
        dma((NX - 1,)),
        dma((NY - 1,)),
        dma((NY - 1,)),
    ]
    input_grad, down_part = pl.pallas_call(
        kernel,
        out_shape=(vmem((tokens, cols), BF16), vmem((rows12, cols), F32)),
        in_specs=[small] * 5 + [big] * 3,
        out_specs=(small, small),
        scratch_shapes=scratch,
        compiler_params=pltpu.CompilerParams(
            collective_id=0, has_side_effects=True, vmem_limit_bytes=LIMIT - 8 * 1024 * 1024
        ),
        name="expert_backward",
    )(*handed, w_gate[0], w_up[0], w_down[0])
    return (input_grad[None], down_part[None])


def solution(mesh):
    in_specs = (
        P("dp", "er", "ec"),
        P("dp", "er"),
        P("dp", "er"),
        P("dp", "er"),
        P("dp", "er", None, None),
        P("dp", "er", None, None),
        P("er", "ec", None),
        P("er", "ec", None),
        P("er", None, "ec"),
    )
    out_specs = (P("dp", "er", "ec"), P("er", "dp", "ec"))
    return jax.shard_map(body, mesh=mesh, in_specs=in_specs, out_specs=out_specs, check_vma=False)
```

```python
import functools

import jax
import jax.numpy as jnp
from jax import lax
from jax.experimental import pallas as pl
from jax.experimental.pallas import tpu as pltpu
from jax.sharding import PartitionSpec as P

MESH = pl.DeviceIdType.MESH
F32, BF16 = jnp.float32, jnp.bfloat16
NX, NY, NC = 4, 8, 2
WAVES = 3
N = 4


def nt(a, b):
    return lax.dot_general(a, b, (((1,), (1,)), ((), ())), preferred_element_type=F32)


def kernel(
    tok_hbm, prob_hbm, ids_hbm, slots_hbm, gate_hbm, up_hbm, wg_hbm, wu_hbm, wd_hbm,
    out_ref, down_ref,
    prob_ref, ids_ref, slots_ref,
    tok, gate, up, wg, wu, wd,
    outbuf, arrived, returned, slotbuf,
    gfac, ufac, hidden, hid_t,
    part, own, relay_in, direct_in, comb, comb_in, hid,
    dn, cin, xs, xin, ysum, ys, yin,
    lsem, disp_s, disp_r, rel_s, rel_r, dir_s, dir_r, com_s, com_r,
    aga_s, aga_r, agb_s, agb_r, agf_s, agf_r, ret_s, ret_r,
    core_s, core_r, x_s, x_r, y_s, y_r,
):
    e, c, p = lax.axis_index("er"), lax.axis_index("ec"), lax.axis_index("dp")
    core, y, x = p % NC, (p // NC) % NY, p // (NC * NY)
    cap = arrived.shape[1]
    piece = part.shape[4]
    half = WAVES * piece
    pieces = [(h, w) for w in range(WAVES) for h in range(2)]

    def columns(h, w):
        return slice(h * half + w * piece, h * half + (w + 1) * piece)

    rows12 = ysum.shape[0] // NY

    def dp_at(x2, y2, core2):
        return (x2 * NY + y2) * NC + core2

    loads = [
        pltpu.make_async_copy(s, d, lsem.at[i])
        for i, (s, d) in enumerate(
            [
                (tok_hbm, tok), (gate_hbm, gate), (up_hbm, up), (wd_hbm, wd), (wg_hbm, wg), (wu_hbm, wu),
                (ids_hbm, ids_ref), (slots_hbm, slots_ref), (prob_hbm, prob_ref),
            ]
        )
    ]
    for i in (6, 7, 8, 0, 1, 2, 3, 4, 5):
        loads[i].start()

    right, left = {"ec": (c + 1) % N}, {"ec": (c + 3) % N}
    partners = [{"er": (e + k) % N} for k in (1, 2, 3)] + [right, left]
    partners += [{"dp": dp_at(x, y, 1 - core)}]
    partners += [{"dp": dp_at((x + k) % NX, y, core)} for k in range(1, NX)]
    partners += [{"dp": dp_at(x, (y + k) % NY, core)} for k in range(1, NY)]
    barrier = pltpu.get_barrier_semaphore()
    for partner in partners:
        pl.semaphore_signal(barrier, inc=1, device_id=partner, device_id_type=MESH)

    def remote(src, dst, s, r, dev):
        return pltpu.make_async_remote_copy(
            src_ref=src, dst_ref=dst, send_sem=s, recv_sem=r, device_id=dev, device_id_type=MESH
        )

    def arriving(ref, r):
        remote(ref, ref, r, r, right).wait_recv()

    tokens = tok.shape[0]
    for i in (6, 7, 8):
        loads[i].wait()
    pos_row = ids_ref[...] * cap + slots_ref[...]
    eye = lax.broadcasted_iota(jnp.int32, (tokens, tokens), 0) == lax.broadcasted_iota(
        jnp.int32, (tokens, tokens), 1
    )

    def as_column(row):
        return jnp.sum(jnp.where(eye, jnp.broadcast_to(row, (tokens, tokens)), 0.0), axis=1, keepdims=True)

    prob_col = as_column(prob_ref[...])
    pos_col = as_column(pos_row.astype(F32))
    loads[0].wait()
    tok[...] = (prob_col * tok[...].astype(F32)).astype(BF16)
    for n, d in enumerate((2, 1, 3, 0)):
        dest = (c + d - e + 2 * N) % N
        k = (dest - e + N) % N
        slot = lax.broadcasted_iota(jnp.int32, (cap, tokens), 0) + dest * cap
        pick = jnp.where(slot == pos_row, 1.0, 0.0).astype(BF16)
        outbuf[d] = jnp.dot(pick, tok[...], preferred_element_type=F32).astype(BF16)
        if n == 0:
            pl.semaphore_wait(barrier, len(partners))

        @pl.when(k == 0)
        def _():
            arrived[e] = outbuf[d]

        @pl.when(k != 0)
        def _():
            remote(outbuf.at[d], arrived.at[e], disp_s.at[k - 1], disp_r.at[k - 1], {"er": dest}).start()

    loads[1].wait()
    loads[2].wait()

    def activations(r, _):
        a, u = gate[r].astype(F32), up[r].astype(F32)
        s = jax.nn.sigmoid(a)
        act = a * s
        ufac[r] = act
        gfac[r] = u * s * (1.0 + a * (1.0 - s))
        hidden[r] = (act * u).astype(BF16)
        return 0

    lax.fori_loop(0, N, activations, 0)
    mrows = hid_t.shape[2]
    width = hidden.shape[2]

    def arrange(q, _):
        row = q * mrows + lax.broadcasted_iota(jnp.int32, (mrows, width), 0)
        other = jnp.where(row >= width // 2, 1, 0)
        rem = row - other * (width // 2)
        group = ((rem.astype(F32) + 0.5) * (1.0 / rows12)).astype(jnp.int32)
        source = rem + rows12 * (group + other)
        pick = jnp.where(source == lax.broadcasted_iota(jnp.int32, (mrows, width), 1), 1.0, 0.0).astype(BF16)
        for r in range(N):
            hid_t[q, r] = nt(pick, hidden[r]).astype(BF16)
        return 0

    lax.fori_loop(0, NX * NC, arrange, 0)

    loads[3].wait()

    def partial(d):
        r = (c + d - e + 2 * N) % N
        k = (e - r + N) % N

        @pl.when(k != 0)
        def _():
            remote(outbuf.at[d], arrived.at[r], disp_s.at[k - 1], disp_r.at[k - 1], {"er": r}).wait_recv()

        return nt(arrived[r], wd[...])

    def keep(d, value):
        for h, w in pieces:
            part[d, h, w] = value[:, columns(h, w)].astype(BF16)

    keep(2, partial(2))
    rel = [
        remote(part.at[2, h, w], relay_in.at[h, w], rel_s.at[h, w], rel_r.at[h, w], (right, left)[h])
        for h, w in pieces
    ]
    for copy in rel:
        copy.start()
    keep(1, partial(1))
    keep(3, partial(3))
    direct = [
        remote(part.at[3 - 2 * h, h, w], direct_in.at[h, w], dir_s.at[h, w], dir_r.at[h, w], (left, right)[h])
        for h, w in pieces
    ]
    for copy in direct:
        copy.start()
    for n, w in pieces:
        h = jnp.where((c == 0) | (c == N - 1), 1 - n, n)
        d = 1 + 2 * h
        arriving(relay_in.at[h, w], rel_r.at[h, w])
        comb[h, w] = (part[d, h, w].astype(F32) + relay_in[h, w].astype(F32)).astype(BF16)
        remote(comb.at[h, w], comb_in.at[h, w], com_s.at[h, w], com_r.at[h, w], {"ec": (c + d) % N}).start()
    combined = [
        remote(comb.at[h, w], comb_in.at[h, w], com_s.at[h, w], com_r.at[h, w], (right, left)[h])
        for h, w in pieces
    ]
    own[...] = partial(0)

    def outer(q, _):
        total = jnp.dot(hid_t[q, 0], arrived[0], preferred_element_type=F32)
        for r in range(1, N):
            total += jnp.dot(hid_t[q, r], arrived[r], preferred_element_type=F32)
        dn[q] = total.astype(BF16)
        return 0

    lax.fori_loop(0, NX * NC, outer, 0)
    swap = remote(
        dn.at[pl.ds((1 - core) * NX, NX)], cin, core_s, core_r, {"dp": dp_at(x, y, 1 - core)}
    )
    swap.start()

    swap.wait_recv()
    for q in range(NX):
        xs[q] = (dn[core * NX + q].astype(F32) + cin[q].astype(F32)).astype(BF16)
    over_x = []
    for k in range(1, NX):
        x2 = (x + k) % NX
        copy = remote(
            xs.at[x2], xin.at[k - 1], x_s.at[k - 1], x_r.at[k - 1], {"dp": dp_at(x2, y, core)}
        )
        copy.start()
        over_x.append(copy)

    first = [
        remote(hid.at[c, h, w], hid.at[c, h, w], aga_s.at[h, w], aga_r.at[h, w], (right, left)[h])
        for h, w in pieces
    ]
    second = [
        remote(hid.at[c, h, w], hid.at[c, h, w], agb_s.at[h, w], agb_r.at[h, w], (left, right)[h])
        for h, w in pieces
    ]
    for i, (h, w) in enumerate(pieces):
        direct[i].wait_recv()
        combined[i].wait_recv()
        total = own[:, columns(h, w)] + direct_in[h, w].astype(F32) + comb_in[h, w].astype(F32)
        hid[c, h, w] = total.astype(BF16)
        first[i].start()
        if h == 1:
            second[i - 1].start()
            second[i].start()

    loads[4].wait()
    loads[5].wait()

    def give_back(d):
        j = (c + d) % N
        r = (j - e + N) % N
        k = (r - e + N) % N
        value = None
        for h in range(2):
            cut = slice(h * half, (h + 1) * half)
            grad = jnp.concatenate([hid[j, h, w] for w in range(WAVES)], axis=1).astype(F32)
            gate_grad = (grad * gfac[r, :, cut]).astype(BF16)
            up_grad = (grad * ufac[r, :, cut]).astype(BF16)
            term = nt(gate_grad, wg[:, cut]) + nt(up_grad, wu[:, cut])
            value = term if value is None else value + term
        slotbuf[d] = value.astype(BF16)

        @pl.when(k == 0)
        def _():
            returned[e] = slotbuf[d]

        @pl.when(k != 0)
        def _():
            send_back(d)

    def send_back(d):
        r = (c + d - e + N) % N
        k = (r - e + N) % N
        remote(slotbuf.at[d], returned.at[e], ret_s.at[k - 1], ret_r.at[k - 1], {"er": r}).start()

    give_back(0)

    for n, w in pieces:
        h = jnp.where((c == 1) | (c == 2), 1 - n, n)
        block = hid.at[(c + 3 - 2 * h + N) % N, h, w]
        arriving(block, aga_r.at[h, w])
        remote(block, block, agf_s.at[h, w], agf_r.at[h, w], {"ec": (c + 1 + 2 * h) % N}).start()
    far = (c + 2) % N
    forward = [
        remote(hid.at[far, h, w], hid.at[far, h, w], agf_s.at[h, w], agf_r.at[h, w], right) for h, w in pieces
    ]
    for copy in over_x:
        copy.wait_recv()
    total = dn[core * NX + x].astype(F32) + cin[x].astype(F32)
    for k in range(NX - 1):
        total += xin[k].astype(F32)
    ysum[...] = total
    for q in range(NY):
        ys[q] = ysum[q * rows12 : (q + 1) * rows12, :].astype(BF16)
    over_y = []
    for k in range(1, NY):
        y2 = (y + k) % NY
        copy = remote(
            ys.at[y2], yin.at[k - 1], y_s.at[k - 1], y_r.at[k - 1], {"dp": dp_at(x, y2, core)}
        )
        copy.start()
        over_y.append(copy)

    for i, (h, _) in enumerate(pieces):
        if h == 0:
            second[i].wait_recv()
    give_back(1)
    for i, (h, _) in enumerate(pieces):
        if h == 1:
            second[i].wait_recv()
    give_back(3)

    for copy in forward:
        copy.wait_recv()
    give_back(2)

    for copy in over_y:
        copy.wait_recv()
    total = ys[y].astype(F32)
    for k in range(NY - 1):
        total += yin[k].astype(F32)
    down_ref[...] = total * (1.0 / (NX * NY * NC))

    pos_lane = pos_col.astype(jnp.int32) - lax.broadcasted_iota(jnp.int32, (tokens, cap), 1)
    result = None
    for k in range(N):
        source = (e - k + N) % N
        if k > 0:
            remote(
                slotbuf.at[0], returned.at[source], ret_s.at[k - 1], ret_r.at[k - 1], {"er": source}
            ).wait_recv()
        pick = jnp.where(pos_lane == source * cap, 1.0, 0.0).astype(BF16)
        term = jnp.dot(pick, returned[source], preferred_element_type=F32)
        result = term if result is None else result + term
    out_ref[...] = result.astype(BF16)

    for k in range(N - 1):
        other = {"er": (e + k + 1) % N}
        remote(outbuf.at[0], arrived.at[e], disp_s.at[k], disp_r.at[k], other).wait_send()
        remote(slotbuf.at[0], returned.at[e], ret_s.at[k], ret_r.at[k], other).wait_send()
    for copy in rel + direct + combined + first + second + forward + over_x + over_y + [swap]:
        copy.wait_send()


def body(out_grad, route_probs, expert_ids, slot_ids, gate_pre, up_act, w_gate, w_up, w_down):
    tokens, cols = out_grad.shape[1:]
    slots, width = gate_pre.shape[2:]
    cap, half = slots // N, width // 2
    mrows = width // (NX * NC)
    rows12 = mrows // NY
    vmem, dma = pltpu.VMEM, pltpu.SemaphoreType.DMA
    scratch = [
        vmem((1, tokens), F32),
        vmem((1, tokens), jnp.int32),
        vmem((1, tokens), jnp.int32),
        vmem((tokens, cols), BF16),
        vmem((N, cap, width), BF16),
        vmem((N, cap, width), BF16),
        vmem((cols, width), BF16),
        vmem((cols, width), BF16),
        vmem((width, cols), BF16),
        vmem((N, cap, cols), BF16),
        vmem((N, cap, cols), BF16),
        vmem((N, cap, cols), BF16),
        vmem((N, cap, cols), BF16),
        vmem((N, cap, width), F32),
        vmem((N, cap, width), F32),
        vmem((N, cap, width), BF16),
        vmem((NX * NC, N, mrows, cap), BF16),
        vmem((N, 2, WAVES, cap, half // WAVES), BF16),
        vmem((cap, width), F32),
        vmem((2, WAVES, cap, half // WAVES), BF16),
        vmem((2, WAVES, cap, half // WAVES), BF16),
        vmem((2, WAVES, cap, half // WAVES), BF16),
        vmem((2, WAVES, cap, half // WAVES), BF16),
        vmem((N, 2, WAVES, cap, half // WAVES), BF16),
        vmem((NX * NC, mrows, cols), BF16),
        vmem((NX, mrows, cols), BF16),
        vmem((NX, mrows, cols), BF16),
        vmem((NX - 1, mrows, cols), BF16),
        vmem((mrows, cols), F32),
        vmem((NY, rows12, cols), BF16),
        vmem((NY - 1, rows12, cols), BF16),
        dma((9,)),
        dma((N - 1,)),
        dma((N - 1,)),
        *[dma((2, WAVES)) for _ in range(12)],
        dma((N - 1,)),
        dma((N - 1,)),
        dma,
        dma,
        dma((NX - 1,)),
        dma((NX - 1,)),
        dma((NY - 1,)),
        dma((NY - 1,)),
    ]
    small = pl.BlockSpec(memory_space=pltpu.VMEM)
    big = pl.BlockSpec(memory_space=pltpu.HBM)
    input_grad, down_part = pl.pallas_call(
        kernel,
        out_shape=(
            pltpu.VMEM((tokens, cols), BF16),
            pltpu.VMEM((rows12, cols), F32),
        ),
        in_specs=[big] * 9,
        out_specs=(small, small),
        scratch_shapes=scratch,
        compiler_params=pltpu.CompilerParams(
            collective_id=0, has_side_effects=True, vmem_limit_bytes=58 * 1024 * 1024
        ),
        name="expert_backward",
    )(
        out_grad[0], route_probs, expert_ids, slot_ids,
        gate_pre.reshape(N, cap, width), up_act.reshape(N, cap, width),
        w_gate[0], w_up[0], w_down[0],
    )
    return (input_grad[None], down_part[None])


def solution(mesh):
    in_specs = (
        P("dp", "er", "ec"),
        P("dp", "er"),
        P("dp", "er"),
        P("dp", "er"),
        P("dp", "er", None, None),
        P("dp", "er", None, None),
        P("er", "ec", None),
        P("er", "ec", None),
        P("er", None, "ec"),
    )
    out_specs = (P("dp", "er", "ec"), P("er", "dp", "ec"))
    return jax.shard_map(body, mesh=mesh, in_specs=in_specs, out_specs=out_specs, check_vma=False)
```
